128 devices in a mesh: dp: 1, tp: 2 (over core), ep: 64 (over z, y, x).
Axes of the slice: x: 4, y: 4, z: 4, core: 2. Of those that a mesh axis runs over, the one named last changes fastest.
Arguments:
- tokens_a: bfloat16 [16384, 2048], P(('dp', 'ep', 'tp'))
- expert_ids_a: int32 [16384, 6], P(('dp', 'ep', 'tp'))
- gates_a: float32 [16384, 6], P(('dp', 'ep', 'tp'))
- tokens_b: bfloat16 [16384, 2048], P(('dp', 'ep', 'tp'))
- expert_ids_b: int32 [16384, 6], P(('dp', 'ep', 'tp'))
- gates_b: float32 [16384, 6], P(('dp', 'ep', 'tp'))
- w_gate: bfloat16 [64, 2048, 1408], P('ep', None, 'tp')
- w_up: bfloat16 [64, 2048, 1408], P('ep', None, 'tp')
- w_down: bfloat16 [64, 1408, 2048], P('ep', 'tp')
Outputs:
- output 1: bfloat16 [16384, 2048], P(('dp', 'ep', 'tp'))
- output 2: bfloat16 [16384, 2048], P(('dp', 'ep', 'tp'))
All inputs are finite; a program needn't handle non-finite values.
Results may differ from the reference program's by a relative error of at most 0.00156.
Values are sent between devices in bfloat16 or wider.
A program may use at most 1 GiB of HBM per device.

```python
import jax
import jax.numpy as jnp
from jax import lax

D_MODEL = 2048
D_FF = 1408
EXPERTS = 64
TOP_K = 6
TOK_DEV = 128
SHARDS = 128

MEAN_LOAD = TOP_K * TOK_DEV // EXPERTS
CAPACITY = MEAN_LOAD + MEAN_LOAD // 4
TOKENS = SHARDS * TOK_DEV
STRIDE = EXPERTS // TOP_K
COPIES = TOK_DEV * TOP_K


def draw_routing(route_key):
    key_perm, key_rand, key_coin = jax.random.split(route_key, 3)
    perm_keys = jax.random.split(key_perm, SHARDS)
    perm_ranks = jax.vmap(lambda one_key: jax.random.permutation(one_key, TOK_DEV))(perm_keys)
    wild_ids = jax.random.randint(key_rand, (SHARDS, TOK_DEV), 0, EXPERTS)
    coin_flip = jax.random.randint(key_coin, (SHARDS, TOK_DEV), 0, 2)
    take_even = (coin_flip == 1) | (perm_ranks < EXPERTS)
    base_ids = jnp.where(take_even, perm_ranks % EXPERTS, wild_ids).reshape(TOKENS)
    offsets = jnp.arange(TOP_K) * STRIDE
    return ((base_ids[:, None] + offsets[None, :]) % EXPERTS).astype(jnp.int32)


def setup_inputs(seed: int = 0, part: int = 0) -> dict:
    part_keys = jax.random.split(jax.random.fold_in(jax.random.key(seed), part), 6)
    weight_keys = jax.random.split(jax.random.key(seed + 1), 3)

    def draw_batch(tok_key, route_key, gate_key):
        tokens = jax.random.normal(tok_key, (TOKENS, D_MODEL), jnp.float32).astype(jnp.bfloat16)
        gate_vals = jax.random.uniform(gate_key, (TOKENS, TOP_K), jnp.float32, 0.25, 1.75) * TOP_K ** -0.5
        return tokens, draw_routing(route_key), gate_vals

    tokens_a, expert_ids_a, gates_a = draw_batch(part_keys[0], part_keys[1], part_keys[2])
    tokens_b, expert_ids_b, gates_b = draw_batch(part_keys[3], part_keys[4], part_keys[5])
    w_gate = (jax.random.normal(weight_keys[0], (EXPERTS, D_MODEL, D_FF), jnp.float32) * D_MODEL ** -0.5).astype(jnp.bfloat16)
    w_up = (jax.random.normal(weight_keys[1], (EXPERTS, D_MODEL, D_FF), jnp.float32) * D_MODEL ** -0.5).astype(jnp.bfloat16)
    w_down = (jax.random.normal(weight_keys[2], (EXPERTS, D_FF, D_MODEL), jnp.float32) * D_FF ** -0.5).astype(jnp.bfloat16)
    return {"tokens_a": tokens_a, "expert_ids_a": expert_ids_a, "gates_a": gates_a, "tokens_b": tokens_b, "expert_ids_b": expert_ids_b, "gates_b": gates_b, "w_gate": w_gate, "w_up": w_up, "w_down": w_down}


def slot_index(flat_ids):
    onehot = (flat_ids[:, None] == jnp.arange(EXPERTS)[None, :]).astype(jnp.int32)
    position = jnp.sum(jnp.cumsum(onehot, axis=0) * onehot, axis=1) - 1
    return jnp.where(position < CAPACITY, flat_ids * CAPACITY + position, EXPERTS * CAPACITY)


def fill_slots(block_rows, slot_ids):
    copy_tok = (jnp.arange(COPIES) // TOP_K).astype(jnp.int32)
    source = jnp.full((EXPERTS * CAPACITY,), TOK_DEV, jnp.int32).at[slot_ids].set(copy_tok, mode="drop")
    return jnp.take(block_rows, source, axis=0, mode="fill", fill_value=0)


def pick_rows(out_rows, slot_ids):
    return jnp.take(out_rows, slot_ids, axis=0, mode="fill", fill_value=0)


def expert_ffn(operands):
    rows_in, gate_w, up_w, down_w = operands
    gate_act = jnp.dot(rows_in, gate_w, preferred_element_type=jnp.float32)
    up_lin = jnp.dot(rows_in, up_w, preferred_element_type=jnp.float32)
    hidden = (jax.nn.silu(gate_act) * up_lin).astype(jnp.bfloat16)
    return jnp.dot(hidden, down_w, preferred_element_type=jnp.float32).astype(jnp.bfloat16)


def moe_layer(tokens, expert_ids, gate_vals, w_gate, w_up, w_down):
    blocks = tokens.reshape(SHARDS, TOK_DEV, D_MODEL)
    flat_ids = expert_ids.reshape(SHARDS, COPIES)
    slot_ids = jax.vmap(slot_index)(flat_ids)
    slot_rows = jax.vmap(fill_slots)(blocks, slot_ids)
    per_expert = slot_rows.reshape(SHARDS, EXPERTS, CAPACITY, D_MODEL).transpose(1, 0, 2, 3).reshape(EXPERTS, SHARDS * CAPACITY, D_MODEL)
    results = lax.map(expert_ffn, (per_expert, w_gate, w_up, w_down))
    back_rows = results.reshape(EXPERTS, SHARDS, CAPACITY, D_MODEL).transpose(1, 0, 2, 3).reshape(SHARDS, EXPERTS * CAPACITY, D_MODEL)
    copies = jax.vmap(pick_rows)(back_rows, slot_ids)
    weighted = copies.reshape(SHARDS, TOK_DEV, TOP_K, D_MODEL).astype(jnp.float32) * gate_vals.reshape(SHARDS, TOK_DEV, TOP_K, 1)
    return jnp.sum(weighted, axis=2).reshape(TOKENS, D_MODEL).astype(jnp.bfloat16)


def reference(tokens_a, expert_ids_a, gates_a, tokens_b, expert_ids_b, gates_b, w_gate, w_up, w_down):
    out_a = moe_layer(tokens_a, expert_ids_a, gates_a, w_gate, w_up, w_down)
    out_b = moe_layer(tokens_b, expert_ids_b, gates_b, w_gate, w_up, w_down)
    return (out_a, out_b)
```

```python
import jax
import jax.numpy as jnp
from jax import lax
from jax.experimental import pallas as pl
from jax.experimental.pallas import tpu as pltpu
from jax.sharding import PartitionSpec as P

MESH_ID = pl.DeviceIdType.MESH
SLOT = 16
CAP = 15
TOK = 128
DIM = 2048
STRIDE = (16, 4, 1)
CHUNKS = ((0, 0, 384), (1, 384, 384), (2, 768, 384), (0, 1152, 384), (1, 1536, 256), (2, 1792, 256))
NCH = len(CHUNKS)


def moe_kernel(tok_a, tok_b, idt, ids_a, ids_b, gate_a, gate_b, wg_in, wu_in, wd_in,
               out_a, out_b, relay_in, relay_out,
               idbuf, gath, send2, rows, turn, fin, wg, wu, wd, sel, comb,
               id_s, id_r, w_s, w_r, w_l, own1,
               d1s, d1r, d2s, d2r, d3s, d3r, r1s, r1r, r2s, r2r, r3s, r3r, own2, own3, own5, own6):
    f32, bf16 = jnp.float32, jnp.bfloat16
    ep = lax.axis_index("ep")
    tp = lax.axis_index("tp")
    me = (ep // 16, lax.rem(ep // 4, 4), lax.rem(ep, 4))
    toks, outs = (tok_a, tok_b), (out_a, out_b)
    ids_n, gates_n = (ids_a, ids_b), (gate_a, gate_b)

    def shifted(axis, step):
        return lax.rem(me[axis] + step, 4)

    def peer(axis, step):
        return {"ep": ep + (shifted(axis, step) - me[axis]) * STRIDE[axis]}

    def remote(src, dst, s_sem, r_sem, dev):
        return pltpu.make_async_remote_copy(src, dst, s_sem, r_sem, device_id=dev, device_id_type=MESH_ID)

    def cols(k):
        return pl.ds(CHUNKS[k][1], CHUNKS[k][2])

    def fixed_canon(buf, bt, axis, at, k):
        if axis == 0:
            return buf.at[bt, at, :, :, :, cols(k)]
        if axis == 1:
            return buf.at[bt, :, at, :, :, cols(k)]
        return buf.at[bt, :, :, at, :, cols(k)]

    def relay_slot(buf, bt, o, k, at):
        if o == 2:
            return buf.at[bt, :, at, :, :, cols(k)]
        return buf.at[bt, :, :, at, :, cols(k)]

    def copy_d1(bt, k, i):
        o = CHUNKS[k][0]
        return remote(toks[bt].at[:, cols(k)], gath.at[bt, me[o], :, cols(k)],
                      d1s.at[bt, k, i - 1], d1r.at[bt, k, i - 1], peer(o, i))

    def local_d1(bt, k):
        o = CHUNKS[k][0]
        return pltpu.make_async_copy(toks[bt].at[:, cols(k)], gath.at[bt, me[o], :, cols(k)], own1.at[bt, k])

    def copy_d2(bt, k, i):
        o = CHUNKS[k][0]
        b = (o + 1) % 3
        return remote(send2.at[shifted(b, i), :, :, :, cols(k)], relay_slot(relay_in, bt, o, k, me[b]),
                      d2s.at[bt, k, i - 1], d2r.at[bt, k, i - 1], peer(b, i))

    def local_d2(bt, k):
        o = CHUNKS[k][0]
        b = (o + 1) % 3
        return pltpu.make_async_copy(send2.at[me[b], :, :, :, cols(k)], relay_slot(relay_in, bt, o, k, me[b]), own2.at[bt, k])

    def copy_3(src, dst, s, r, bt, k, i):
        c = (CHUNKS[k][0] + 2) % 3
        return remote(src.at[bt, shifted(c, i), :, :, :, cols(k)], fixed_canon(dst, bt, c, me[c], k),
                      s.at[bt, k, i - 1], r.at[bt, k, i - 1], peer(c, i))

    def local_3(src, dst, sem, bt, k):
        c = (CHUNKS[k][0] + 2) % 3
        return pltpu.make_async_copy(src.at[bt, me[c], :, :, :, cols(k)], fixed_canon(dst, bt, c, me[c], k), sem.at[bt, k])

    def copy_r1(bt, k, i):
        o = CHUNKS[k][0]
        return remote(fixed_canon(rows, bt, o, shifted(o, i), k), turn.at[bt, :, :, me[o], :, cols(k)],
                      r1s.at[bt, k, i - 1], r1r.at[bt, k, i - 1], peer(o, i))

    def turn_part(bt, k, at):
        if CHUNKS[k][0] == 1:
            return turn.at[bt, :, at, :, :, cols(k)]
        return turn.at[bt, at, :, :, :, cols(k)]

    def copy_r2(bt, k, i):
        o = CHUNKS[k][0]
        b = (o + 1) % 3
        return remote(turn_part(bt, k, shifted(b, i)), relay_slot(relay_out, bt, o, k, me[b]),
                      r2s.at[bt, k, i - 1], r2r.at[bt, k, i - 1], peer(b, i))

    def local_r2(bt, k):
        o = CHUNKS[k][0]
        b = (o + 1) % 3
        return pltpu.make_async_copy(turn_part(bt, k, me[b]), relay_slot(relay_out, bt, o, k, me[b]), own5.at[bt, k])

    def copy_d3(bt, k, i):
        return copy_3(relay_in, rows, d3s, d3r, bt, k, i)

    def copy_r3(bt, k, i):
        return copy_3(relay_out, fin, r3s, r3r, bt, k, i)

    def local_d3(bt, k):
        return local_3(relay_in, rows, own3, bt, k)

    def local_r3(bt, k):
        return local_3(relay_out, fin, own6, bt, k)

    def start3(copy, bt, k):
        for i in (2, 1, 3):
            copy(bt, k, i).start()

    def recv3(copy, bt, k):
        for i in (1, 3, 2):
            copy(bt, k, i).wait_recv()

    def sent3(copy, bt, k):
        for i in (1, 2, 3):
            copy(bt, k, i).wait_send()

    barrier = pltpu.get_barrier_semaphore()
    for axis in range(3):
        for i in (1, 2, 3):
            pl.semaphore_signal(barrier, inc=1, device_id=peer(axis, i), device_id_type=MESH_ID)
    other = {"tp": 1 - tp}
    pl.semaphore_signal(barrier, inc=1, device_id=other, device_id_type=MESH_ID)
    for bt in (0, 1):
        for k in range(NCH):
            local_d1(bt, k).start()
    weights = ((wg_in, wg), (wu_in, wu), (wd_in, wd))

    def weight_local(n):
        src, dst = weights[n]
        return pltpu.make_async_copy(src.at[0], dst.at[tp], w_l.at[n])

    def weight_remote(n):
        src, dst = weights[n]
        return remote(src.at[0], dst.at[tp], w_s.at[n], w_r.at[n], other)

    def id_copy(axis, i):
        return remote(idt, idbuf.at[axis, me[axis]], id_s.at[axis, i - 1], id_r.at[axis, i - 1], peer(axis, i))

    for n in range(3):
        weight_local(n).start()
    for axis in range(3):
        idbuf[axis, me[axis]] = idt[...]

    pl.semaphore_wait(barrier, 10)
    for axis in range(3):
        for i in (2, 1, 3):
            id_copy(axis, i).start()
    for k in range(NCH):
        start3(copy_d1, 0, k)
    for n in range(3):
        weight_remote(n).start()

    def iota(shape, dim):
        return lax.broadcasted_iota(jnp.int32, shape, dim)

    def build_comb(bt):
        ids, gates = ids_n[bt][...], gates_n[bt][...]
        expert = iota((TOK, 64), 1)
        hit = jnp.zeros((TOK, 64), f32)
        gate = jnp.zeros((TOK, 64), f32)
        for j in range(ids.shape[1]):
            same = ids[:, j:j + 1] == expert
            hit = jnp.where(same, 1.0, hit)
            gate = jnp.where(same, gates[:, j:j + 1], gate)
        before = jnp.where(iota((TOK, TOK), 1) < iota((TOK, TOK), 0), 1.0, 0.0).astype(bf16)
        count = jnp.dot(before, hit.astype(bf16), preferred_element_type=f32)
        place = jnp.where((hit > 0.5) & (count < CAP - 0.5), count, -1.0)
        spread = jnp.where(iota((64, 64 * SLOT), 1) // SLOT == iota((64, 64 * SLOT), 0), 1.0, 0.0).astype(bf16)
        wide = jnp.dot(place.astype(bf16), spread, preferred_element_type=f32)
        at_slot = wide == lax.rem(iota((TOK, 64 * SLOT), 1), SLOT).astype(f32)
        rest = gate
        for n in range(3):
            part = rest.astype(bf16)
            rest = rest - part.astype(f32)
            part_wide = jnp.dot(part, spread, preferred_element_type=f32)
            comb[bt, n * TOK:(n + 1) * TOK, :] = jnp.where(at_slot, part_wide, 0.0).astype(bf16)

    def build_sel(bt):
        before = jnp.where(iota((TOK, TOK), 0) < iota((TOK, TOK), 1), 1.0, 0.0).astype(bf16)
        for o in range(3):
            b, c = (o + 1) % 3, (o + 2) % 3
            row = iota((16, TOK), 0)
            expert = me[o] * STRIDE[o] + (row // 4) * STRIDE[b] + lax.rem(row, 4) * STRIDE[c]
            for a in range(4):
                ids = idbuf[o, a, bt * 8:bt * 8 + 8, :]
                hit = jnp.zeros((16, TOK), f32)
                for j in range(6):
                    hit = jnp.where(ids[j:j + 1, :] == expert, 1.0, hit)
                count = jnp.dot(hit.astype(bf16), before, preferred_element_type=f32)
                place = jnp.where((hit > 0.5) & (count < CAP - 0.5), count, -1.0)
                slot = iota((SLOT, TOK), 0).astype(f32)
                for r in range(16):
                    sel[bt, o, a, r * SLOT:(r + 1) * SLOT, :] = jnp.where(place[r:r + 1, :] == slot, 1.0, 0.0).astype(bf16)

    def step_d2(bt, k):
        o, c0, w = CHUNKS[k]
        local_d1(bt, k).wait()
        recv3(copy_d1, bt, k)
        if bt == 1:
            sent3(copy_d2, 0, k)
        for a in range(4):
            got = jnp.dot(sel[bt, o, a], gath[bt, a, :, c0:c0 + w], preferred_element_type=f32)
            send2[:, :, a, :, c0:c0 + w] = got.astype(bf16).reshape(4, 4, SLOT, w)
        start3(copy_d2, bt, k)
        local_d2(bt, k).start()

    def step_d3(bt, k):
        local_d2(bt, k).wait()
        recv3(copy_d2, bt, k)
        start3(copy_d3, bt, k)
        local_d3(bt, k).start()

    def wait_rows(bt):
        for k in range(NCH):
            recv3(copy_d3, bt, k)
            local_d3(bt, k).wait()

    def ffn(bt, m):
        x = rows[bt, m].reshape(256, DIM)
        total = None
        for h in (0, 1):
            g = jnp.dot(x, wg[h], preferred_element_type=f32)
            u = jnp.dot(x, wu[h], preferred_element_type=f32)
            hid = (jax.nn.silu(g) * u).astype(bf16)
            part = jnp.dot(hid, wd[h], preferred_element_type=f32)
            total = part if total is None else total + part
        rows[bt, m] = total.astype(bf16).reshape(4, 4, SLOT, DIM)

    def step_r1(bt):
        for k in range(NCH):
            start3(copy_r1, bt, k)
        for k in range(NCH):
            o, c0, w = CHUNKS[k]
            cs = slice(c0, c0 + w)
            if o == 0:
                turn[bt, :, :, me[0], :, cs] = rows[bt, me[0], :, :, :, cs]
            elif o == 1:
                turn[bt, :, :, me[1], :, cs] = rows[bt, :, me[1], :, :, cs]
            else:
                turn[bt, :, :, me[2], :, cs] = rows[bt, :, :, me[2], :, cs]

    def step_r2(bt, k):
        recv3(copy_r1, bt, k)
        start3(copy_r2, bt, k)
        local_r2(bt, k).start()

    def step_r3(bt, k):
        recv3(copy_r2, bt, k)
        local_r2(bt, k).wait()
        start3(copy_r3, bt, k)
        local_r3(bt, k).start()

    def step_out(bt, k):
        o, c0, w = CHUNKS[k]
        recv3(copy_r3, bt, k)
        local_r3(bt, k).wait()
        vals = fin[bt, :, :, :, :, c0:c0 + w].reshape(64 * SLOT, w)
        got = jnp.dot(comb[bt], vals, preferred_element_type=f32)
        outs[bt][:, c0:c0 + w] = (got[:TOK] + got[TOK:2 * TOK] + got[2 * TOK:]).astype(bf16)

    for axis in range(3):
        for i in (1, 3, 2):
            id_copy(axis, i).wait_recv()
    build_sel(0)
    step_d2(0, 0)
    step_d2(0, 1)
    step_d2(0, 2)
    for k in range(NCH):
        start3(copy_d1, 1, k)
    for k in range(3):
        step_d2(0, k + 3)
        step_d3(0, k)
    build_sel(1)
    for k in range(3):
        step_d3(0, k + 3)
        step_d2(1, k)
    for n in range(3):
        weight_local(n).wait()
        weight_remote(n).wait_recv()
    wait_rows(0)

    after = {
        0: [lambda: step_d2(1, 3), lambda: step_d2(1, 4), lambda: step_d2(1, 5), lambda: step_d3(1, 0)],
        1: [lambda: step_d3(1, 1), lambda: step_d3(1, 2), lambda: step_d3(1, 3)],
        2: [lambda: step_d3(1, 4), lambda: step_d3(1, 5), lambda: build_comb(0), lambda: build_comb(1)],
        3: [lambda: step_r1(0), lambda: wait_rows(1)],
        4: [lambda: step_r2(0, 0), lambda: step_r2(0, 1), lambda: step_r2(0, 2)],
        5: [lambda: step_r2(0, 3), lambda: step_r2(0, 4), lambda: step_r2(0, 5), lambda: step_r3(0, 0)],
        6: [lambda: step_r3(0, 1), lambda: step_r3(0, 2), lambda: step_r3(0, 3)],
        7: [lambda: step_r1(1), lambda: step_r3(0, 4), lambda: step_r3(0, 5)],
    }

    def loop(step, carry):
        ffn(step // 4, lax.rem(step, 4))
        for at, todo in after.items():
            @pl.when(step == at)
            def _():
                for one in todo:
                    one()
        return carry

    lax.fori_loop(0, 8, loop, 0)

    for k in range(NCH):
        step_r2(1, k)
        step_out(0, k)
        if k >= 1:
            step_r3(1, k - 1)
    step_r3(1, NCH - 1)
    for k in range(NCH):
        step_out(1, k)

    for axis in range(3):
        for i in (1, 2, 3):
            id_copy(axis, i).wait_send()
    for n in range(3):
        weight_remote(n).wait_send()
    for bt in (0, 1):
        for k in range(NCH):
            sent3(copy_d1, bt, k)
            if bt == 1:
                sent3(copy_d2, bt, k)
            sent3(copy_d3, bt, k)
            sent3(copy_r1, bt, k)
            sent3(copy_r2, bt, k)
            sent3(copy_r3, bt, k)


def solution(mesh):
    row_spec = P(("dp", "ep", "tp"), None)
    gate_spec = P("ep", None, "tp")
    down_spec = P("ep", "tp", None)
    bf16 = jnp.bfloat16
    dma = pltpu.SemaphoreType.DMA

    def body(tok_a, ids_a, gate_a, tok_b, ids_b, gate_b, wg, wu, wd):
        pad = ((0, 2), (0, 0))
        idt = jnp.concatenate([jnp.pad(ids_a.T, pad, constant_values=-1), jnp.pad(ids_b.T, pad, constant_values=-1)])
        vmem = pl.BlockSpec(memory_space=pltpu.VMEM)
        hbm = pl.BlockSpec(memory_space=pl.ANY)
        half = wg.shape[2]
        box = (2, 4, 4, 4, SLOT, DIM)
        out = jax.ShapeDtypeStruct((TOK, DIM), bf16)
        relay = jax.ShapeDtypeStruct(box, bf16)
        stage = [dma((2, NCH, 3))] * 12
        res = pl.pallas_call(
            moe_kernel,
            out_shape=(out, out, relay, relay),
            in_specs=[hbm, hbm, vmem, vmem, vmem, vmem, vmem, hbm, hbm, hbm],
            out_specs=(vmem, vmem, hbm, hbm),
            scratch_shapes=[
                pltpu.VMEM((3, 4, 16, TOK), jnp.int32),
                pltpu.VMEM((2, 4, TOK, DIM), bf16),
                pltpu.VMEM((4, 4, 4, SLOT, DIM), bf16),
                pltpu.VMEM(box, bf16),
                pltpu.VMEM(box, bf16),
                pltpu.VMEM(box, bf16),
                pltpu.VMEM((2, DIM, half), bf16),
                pltpu.VMEM((2, DIM, half), bf16),
                pltpu.VMEM((2, half, DIM), bf16),
                pltpu.VMEM((2, 3, 4, 256, TOK), bf16),
                pltpu.VMEM((2, 3 * TOK, 64 * SLOT), bf16),
                dma((3, 3)), dma((3, 3)), dma((3,)), dma((3,)), dma((3,)), dma((2, NCH)),
                *stage,
                dma((2, NCH)), dma((2, NCH)), dma((2, NCH)), dma((2, NCH)),
            ],
            compiler_params=pltpu.CompilerParams(collective_id=0, has_side_effects=True, vmem_limit_bytes=67043328),
            name="moe",
        )(tok_a, tok_b, idt, ids_a, ids_b, gate_a, gate_b, wg, wu, wd)
        return res[0], res[1]

    specs = (row_spec,) * 6 + (gate_spec, gate_spec, down_spec)
    return jax.shard_map(body, mesh=mesh, in_specs=specs, out_specs=(row_spec, row_spec), check_vma=False)
```

```python
import jax
import jax.numpy as jnp
from jax import lax
from jax.experimental import pallas as pl
from jax.experimental.pallas import tpu as pltpu
from jax.sharding import PartitionSpec as P

MESH_ID = pl.DeviceIdType.MESH
SLOT = 16
CAP = 15
TOK = 128
DIM = 2048
STRIDE = (16, 4, 1)
CHUNKS = ((0, 0, 384), (1, 384, 384), (2, 768, 384), (0, 1152, 384), (1, 1536, 256), (2, 1792, 256))
NCH = len(CHUNKS)
BEFORE = (
    ("D1", 0, 4), ("D1", 0, 2), ("D1", 0, 1), ("D1", 0, 3), ("D1", 0, 5), ("D1", 0, 0),
    ("S", 0, 0), ("D1", 1, 2), ("D1", 1, 4), ("D1", 1, 3), ("D1", 1, 1), ("D1", 1, 5),
    ("D2", 0, 4), ("D2", 0, 2), ("D2", 0, 5), ("D2", 0, 0), ("D2", 0, 1), ("S", 1, 0),
    ("D2", 0, 3), ("D3", 0, 4), ("D1", 1, 0), ("D3", 0, 0), ("D3", 0, 2), ("D3", 0, 3),
    ("D3", 0, 1), ("D2", 1, 4), ("D2", 1, 2), ("D3", 0, 5), ("W", 0, 0), ("D2", 1, 0),
    ("D2", 1, 3), ("D2", 1, 1),
)
WHILE = {
    2: (("D2", 1, 5), ("D3", 1, 0), ("D3", 1, 2), ("D3", 1, 4),),
    7: (("D3", 1, 1), ("D3", 1, 3), ("D3", 1, 5),),
    11: (("R1", 0, 2), ("R1", 0, 0), ("R1", 0, 4), ("R1", 0, 1),),
    13: (("R1", 0, 3), ("R1", 0, 5), ("R2", 0, 4),),
    14: (("R2", 0, 0),),
    15: (("R2", 0, 2),),
    19: (("R2", 0, 3), ("R2", 0, 1),),
    21: (("R2", 0, 5),),
    22: (("R3", 0, 2), ("R3", 0, 4), ("R3", 0, 0),),
}
AFTER = (
    ("R1", 1, 3), ("R1", 1, 1), ("R1", 1, 2), ("R1", 1, 0), ("R3", 0, 1), ("W", 1, 0),
    ("R3", 0, 3), ("R1", 1, 5), ("C", 0, 4), ("R1", 1, 4), ("R2", 1, 2), ("R2", 1, 3),
    ("R2", 1, 0), ("C", 0, 3), ("R2", 1, 1), ("R2", 1, 4), ("R3", 0, 5), ("R3", 1, 3),
    ("R2", 1, 5), ("R3", 1, 2), ("R3", 1, 1), ("C", 0, 1), ("R3", 1, 4), ("R3", 1, 5),
    ("R3", 1, 0), ("C", 0, 0), ("C", 0, 5), ("C", 1, 3), ("C", 0, 2), ("C", 1, 1),
    ("C", 1, 2), ("C", 1, 4), ("C", 1, 5), ("C", 1, 0),
)


def moe_kernel(tok_a, tok_b, ids_a, ids_b, gate_a, gate_b, wg_in, wu_in, wd_in,
               out, relay_in, relay_out,
               idbuf, gath, send2, rows, turn, fin, wg, wu, wd, hid, sel, comb,
               id_s, id_r, w_s, w_r, w_l, own1,
               d1s, d1r, d2s, d2r, d3s, d3r, r1s, r1r, r2s, r2r, r3s, r3r, own2, own3, own5, own6):
    f32, bf16 = jnp.float32, jnp.bfloat16
    ep = lax.axis_index("ep")
    tp = lax.axis_index("tp")
    me = (ep // 16, lax.rem(ep // 4, 4), lax.rem(ep, 4))
    toks = (tok_a, tok_b)
    ids_n, gates_n = (ids_a, ids_b), (gate_a, gate_b)

    def shifted(axis, step):
        return lax.rem(me[axis] + step, 4)

    def peer(axis, step):
        return {"ep": ep + (shifted(axis, step) - me[axis]) * STRIDE[axis]}

    def remote(src, dst, s_sem, r_sem, dev):
        return pltpu.make_async_remote_copy(src, dst, s_sem, r_sem, device_id=dev, device_id_type=MESH_ID)

    def cols(k):
        return pl.ds(CHUNKS[k][1], CHUNKS[k][2])

    def fixed_canon(buf, bt, axis, at, k):
        if axis == 0:
            return buf.at[bt, at, :, :, :, cols(k)]
        if axis == 1:
            return buf.at[bt, :, at, :, :, cols(k)]
        return buf.at[bt, :, :, at, :, cols(k)]

    def relay_slot(buf, bt, o, k, at):
        if o == 2:
            return buf.at[bt, :, at, :, :, cols(k)]
        return buf.at[bt, :, :, at, :, cols(k)]

    def copy_d1(bt, k, i):
        o = CHUNKS[k][0]
        return remote(toks[bt].at[:, cols(k)], gath.at[bt, me[o], :, cols(k)],
                      d1s.at[bt, k, i - 1], d1r.at[bt, k, i - 1], peer(o, i))

    def local_d1(bt, k):
        o = CHUNKS[k][0]
        return pltpu.make_async_copy(toks[bt].at[:, cols(k)], gath.at[bt, me[o], :, cols(k)], own1.at[bt, k])

    def copy_d2(bt, k, i):
        o = CHUNKS[k][0]
        b = (o + 1) % 3
        return remote(send2.at[shifted(b, i), :, :, :, cols(k)], relay_slot(relay_in, bt, o, k, me[b]),
                      d2s.at[bt, k, i - 1], d2r.at[bt, k, i - 1], peer(b, i))

    def local_d2(bt, k):
        o = CHUNKS[k][0]
        b = (o + 1) % 3
        return pltpu.make_async_copy(send2.at[me[b], :, :, :, cols(k)], relay_slot(relay_in, bt, o, k, me[b]), own2.at[bt, k])

    def copy_3(src, dst, s, r, bt, k, i):
        c = (CHUNKS[k][0] + 2) % 3
        return remote(src.at[bt, shifted(c, i), :, :, :, cols(k)], fixed_canon(dst, bt, c, me[c], k),
                      s.at[bt, k, i - 1], r.at[bt, k, i - 1], peer(c, i))

    def local_3(src, dst, sem, bt, k):
        c = (CHUNKS[k][0] + 2) % 3
        return pltpu.make_async_copy(src.at[bt, me[c], :, :, :, cols(k)], fixed_canon(dst, bt, c, me[c], k), sem.at[bt, k])

    def copy_r1(bt, k, i):
        o = CHUNKS[k][0]
        return remote(fixed_canon(rows, bt, o, shifted(o, i), k), turn.at[bt, :, :, me[o], :, cols(k)],
                      r1s.at[bt, k, i - 1], r1r.at[bt, k, i - 1], peer(o, i))

    def turn_part(bt, k, at):
        if CHUNKS[k][0] == 1:
            return turn.at[bt, :, at, :, :, cols(k)]
        return turn.at[bt, at, :, :, :, cols(k)]

    def copy_r2(bt, k, i):
        o = CHUNKS[k][0]
        b = (o + 1) % 3
        return remote(turn_part(bt, k, shifted(b, i)), relay_slot(relay_out, bt, o, k, me[b]),
                      r2s.at[bt, k, i - 1], r2r.at[bt, k, i - 1], peer(b, i))

    def local_r2(bt, k):
        o = CHUNKS[k][0]
        b = (o + 1) % 3
        return pltpu.make_async_copy(turn_part(bt, k, me[b]), relay_slot(relay_out, bt, o, k, me[b]), own5.at[bt, k])

    def copy_d3(bt, k, i):
        return copy_3(relay_in, rows, d3s, d3r, bt, k, i)

    def copy_r3(bt, k, i):
        return copy_3(relay_out, fin, r3s, r3r, bt, k, i)

    def local_d3(bt, k):
        return local_3(relay_in, rows, own3, bt, k)

    def local_r3(bt, k):
        return local_3(relay_out, fin, own6, bt, k)

    def start3(copy, bt, k):
        for i in (2, 1, 3):
            copy(bt, k, i).start()

    def recv3(copy, bt, k):
        for i in (1, 3, 2):
            copy(bt, k, i).wait_recv()

    def sent3(copy, bt, k):
        for i in (1, 2, 3):
            copy(bt, k, i).wait_send()

    barrier = pltpu.get_barrier_semaphore()
    for axis in range(3):
        for i in (1, 2, 3):
            pl.semaphore_signal(barrier, inc=1, device_id=peer(axis, i), device_id_type=MESH_ID)
    other = {"tp": 1 - tp}
    pl.semaphore_signal(barrier, inc=1, device_id=other, device_id_type=MESH_ID)
    for bt in (0, 1):
        for k in range(NCH):
            local_d1(bt, k).start()
    weights = ((wg_in, wg), (wu_in, wu), (wd_in, wd))

    def weight_local(n):
        src, dst = weights[n]
        return pltpu.make_async_copy(src.at[0], dst.at[tp], w_l.at[n])

    def weight_remote(n):
        src, dst = weights[n]
        return remote(src.at[0], dst.at[tp], w_s.at[n], w_r.at[n], other)

    def id_copy(axis, i):
        return remote(idbuf.at[axis, me[axis]], idbuf.at[axis, me[axis]], id_s.at[axis, i - 1], id_r.at[axis, i - 1], peer(axis, i))

    for n in range(3):
        weight_local(n).start()
    for axis in range(3):
        idbuf[axis, me[axis]] = jnp.full((16, TOK), -1, jnp.int32)
        for bt in (0, 1):
            idbuf[axis, me[axis], bt * 8:bt * 8 + 6, :] = ids_n[bt][...]

    pl.semaphore_wait(barrier, 10)
    for axis in range(3):
        for i in (2, 1, 3):
            id_copy(axis, i).start()

    def iota(shape, dim):
        return lax.broadcasted_iota(jnp.int32, shape, dim)

    def build_comb(bt):
        ids, gates = ids_n[bt][...], gates_n[bt][...]
        expert = iota((64, TOK), 0)
        hit = jnp.zeros((64, TOK), f32)
        gate = jnp.zeros((64, TOK), f32)
        for j in range(6):
            same = ids[j:j + 1, :] == expert
            hit = jnp.where(same, 1.0, hit)
            gate = jnp.where(same, gates[j:j + 1, :], gate)
        before = jnp.where(iota((TOK, TOK), 0) < iota((TOK, TOK), 1), 1.0, 0.0).astype(bf16)
        count = jnp.dot(hit.astype(bf16), before, preferred_element_type=f32)
        place = jnp.transpose(jnp.where((hit > 0.5) & (count < CAP - 0.5), count, -1.0))
        gate = jnp.transpose(gate)
        spread = jnp.where(iota((64, 64 * SLOT), 1) // SLOT == iota((64, 64 * SLOT), 0), 1.0, 0.0).astype(bf16)
        wide = jnp.dot(place.astype(bf16), spread, preferred_element_type=f32)
        at_slot = wide == lax.rem(iota((TOK, 64 * SLOT), 1), SLOT).astype(f32)
        rest = gate
        for n in range(3):
            part = rest.astype(bf16)
            rest = rest - part.astype(f32)
            part_wide = jnp.dot(part, spread, preferred_element_type=f32)
            comb[bt, n * TOK:(n + 1) * TOK, :] = jnp.where(at_slot, part_wide, 0.0).astype(bf16)

    def build_sel(bt):
        before = jnp.where(iota((TOK, TOK), 0) < iota((TOK, TOK), 1), 1.0, 0.0).astype(bf16)
        for o in range(3):
            b, c = (o + 1) % 3, (o + 2) % 3
            row = iota((16, TOK), 0)
            expert = me[o] * STRIDE[o] + (row // 4) * STRIDE[b] + lax.rem(row, 4) * STRIDE[c]
            for a in range(4):
                ids = idbuf[o, a, bt * 8:bt * 8 + 8, :]
                hit = jnp.zeros((16, TOK), f32)
                for j in range(6):
                    hit = jnp.where(ids[j:j + 1, :] == expert, 1.0, hit)
                count = jnp.dot(hit.astype(bf16), before, preferred_element_type=f32)
                place = jnp.where((hit > 0.5) & (count < CAP - 0.5), count, -1.0)
                slot = iota((SLOT, TOK), 0).astype(f32)
                for r in range(16):
                    sel[bt, o, a, r * SLOT:(r + 1) * SLOT, :] = jnp.where(place[r:r + 1, :] == slot, 1.0, 0.0).astype(bf16)

    def step_d2(bt, k):
        o, c0, w = CHUNKS[k]
        local_d1(bt, k).wait()
        recv3(copy_d1, bt, k)
        if bt == 1:
            sent3(copy_d2, 0, k)
        for a in range(4):
            got = jnp.dot(sel[bt, o, a], gath[bt, a, :, c0:c0 + w], preferred_element_type=f32)
            send2[:, :, a, :, c0:c0 + w] = got.astype(bf16).reshape(4, 4, SLOT, w)
        start3(copy_d2, bt, k)
        local_d2(bt, k).start()

    def step_d3(bt, k):
        local_d2(bt, k).wait()
        recv3(copy_d2, bt, k)
        start3(copy_d3, bt, k)
        local_d3(bt, k).start()

    def wait_rows(bt):
        for k in range(NCH):
            recv3(copy_d3, bt, k)
            local_d3(bt, k).wait()

    def expert_step(step):
        bt, part = step // 12, lax.rem(step, 3)
        m = lax.rem(step, 12) // 3

        @pl.when(part < 2)
        def _():
            x = rows[bt, m].reshape(256, DIM)
            g = lax.dot_general(x, wg[part], (((1,), (1,)), ((), ())), preferred_element_type=f32)
            u = lax.dot_general(x, wu[part], (((1,), (1,)), ((), ())), preferred_element_type=f32)
            hid[part] = (jax.nn.silu(g) * u).astype(bf16)

        @pl.when(part == 2)
        def _():
            total = jnp.dot(hid[0], wd[0], preferred_element_type=f32)
            total = total + jnp.dot(hid[1], wd[1], preferred_element_type=f32)
            rows[bt, m] = total.astype(bf16).reshape(4, 4, SLOT, DIM)

    def step_d1(bt, k):
        start3(copy_d1, bt, k)

    def step_r1(bt, k):
        start3(copy_r1, bt, k)
        o, c0, w = CHUNKS[k]
        cs = slice(c0, c0 + w)
        if o == 0:
            turn[bt, :, :, me[0], :, cs] = rows[bt, me[0], :, :, :, cs]
        elif o == 1:
            turn[bt, :, :, me[1], :, cs] = rows[bt, :, me[1], :, :, cs]
        else:
            turn[bt, :, :, me[2], :, cs] = rows[bt, :, :, me[2], :, cs]

    def step_r2(bt, k):
        recv3(copy_r1, bt, k)
        start3(copy_r2, bt, k)
        local_r2(bt, k).start()

    def step_r3(bt, k):
        recv3(copy_r2, bt, k)
        local_r2(bt, k).wait()
        start3(copy_r3, bt, k)
        local_r3(bt, k).start()

    def step_out(bt, k):
        o, c0, w = CHUNKS[k]
        recv3(copy_r3, bt, k)
        local_r3(bt, k).wait()
        vals = fin[bt, :, :, :, :, c0:c0 + w].reshape(64 * SLOT, w)
        got = jnp.dot(comb[bt], vals, preferred_element_type=f32)
        out[bt, :, c0:c0 + w] = (got[:TOK] + got[TOK:2 * TOK] + got[2 * TOK:]).astype(bf16)

    todo = {"D1": step_d1, "D2": step_d2, "D3": step_d3, "R1": step_r1, "R2": step_r2, "R3": step_r3, "C": step_out,
            "S": lambda bt, k: build_sel(bt), "W": lambda bt, k: build_comb(bt)}

    def run(steps):
        for name, bt, k in steps:
            if (name, bt) == ("S", 0):
                for n in range(3):
                    weight_remote(n).start()
                for axis in range(3):
                    for i in (1, 3, 2):
                        id_copy(axis, i).wait_recv()
            todo[name](bt, k)

    run(BEFORE)
    for n in range(3):
        weight_local(n).wait()
        weight_remote(n).wait_recv()
    wait_rows(0)

    def loop(step, carry):
        @pl.when(step == 12)
        def _():
            wait_rows(1)

        expert_step(step)
        for at, steps in WHILE.items():
            @pl.when(step == at)
            def _():
                run(steps)
        return carry

    lax.fori_loop(0, 24, loop, 0)
    run(AFTER)

    for axis in range(3):
        for i in (1, 2, 3):
            id_copy(axis, i).wait_send()
    for n in range(3):
        weight_remote(n).wait_send()
    for bt in (0, 1):
        for k in range(NCH):
            sent3(copy_d1, bt, k)
            if bt == 1:
                sent3(copy_d2, bt, k)
            sent3(copy_d3, bt, k)
            sent3(copy_r1, bt, k)
            sent3(copy_r2, bt, k)
            sent3(copy_r3, bt, k)


def solution(mesh):
    row_spec = P(("dp", "ep", "tp"), None)
    gate_spec = P("ep", None, "tp")
    down_spec = P("ep", "tp", None)
    bf16 = jnp.bfloat16
    dma = pltpu.SemaphoreType.DMA

    def body(tok_a, ids_a, gate_a, tok_b, ids_b, gate_b, wg, wu, wd):
        vmem = pl.BlockSpec(memory_space=pltpu.VMEM)
        hbm = pl.BlockSpec(memory_space=pl.ANY)
        half = wd.shape[1]
        box = (2, 4, 4, 4, SLOT, DIM)
        out = jax.ShapeDtypeStruct((TOK, DIM), bf16)
        relay = jax.ShapeDtypeStruct(box, bf16)
        stage = [dma((2, NCH, 3))] * 12
        res = pl.pallas_call(
            moe_kernel,
            out_shape=(jax.ShapeDtypeStruct((2, TOK, DIM), bf16), relay, relay),
            in_specs=[hbm, hbm, vmem, vmem, vmem, vmem, hbm, hbm, hbm],
            out_specs=(vmem, hbm, hbm),
            scratch_shapes=[
                pltpu.VMEM((3, 4, 16, TOK), jnp.int32),
                pltpu.VMEM((2, 4, TOK, DIM), bf16),
                pltpu.VMEM((4, 4, 4, SLOT, DIM), bf16),
                pltpu.VMEM(box, bf16),
                pltpu.VMEM(box, bf16),
                pltpu.VMEM(box, bf16),
                pltpu.VMEM((2, half, DIM), bf16),
                pltpu.VMEM((2, half, DIM), bf16),
                pltpu.VMEM((2, half, DIM), bf16),
                pltpu.VMEM((2, 256, half), bf16),
                pltpu.VMEM((2, 3, 4, 256, TOK), bf16),
                pltpu.VMEM((2, 3 * TOK, 64 * SLOT), bf16),
                dma((3, 3)), dma((3, 3)), dma((3,)), dma((3,)), dma((3,)), dma((2, NCH)),
                *stage,
                dma((2, NCH)), dma((2, NCH)), dma((2, NCH)), dma((2, NCH)),
            ],
            compiler_params=pltpu.CompilerParams(collective_id=0, has_side_effects=True, vmem_limit_bytes=67043328),
            name="moe",
        )(tok_a, tok_b, ids_a.T, ids_b.T, gate_a.T, gate_b.T, wg.transpose(0, 2, 1), wu.transpose(0, 2, 1), wd)
        return res[0][0], res[0][1]

    specs = (row_spec,) * 6 + (gate_spec, gate_spec, down_spec)
    return jax.shard_map(body, mesh=mesh, in_specs=specs, out_specs=(row_spec, row_spec), check_vma=False)
```

```python
import jax
import jax.numpy as jnp
from jax import lax
from jax.experimental import pallas as pl
from jax.experimental.pallas import tpu as pltpu
from jax.sharding import PartitionSpec as P

MESH_ID = pl.DeviceIdType.MESH
SLOT = 16
CAP = 15
TOK = 128
DIM = 2048
MAIN = 1920
LANE = 128
STRIDE = (16, 4, 1)
FINE = ((0, 0, 384), (1, 384, 384), (2, 768, 384), (0, 1152, 256), (1, 1408, 256), (2, 1664, 256))
COARSE = ((0, 0, 640), (1, 640, 640), (2, 1280, 640))
IN, OUT = (FINE, FINE), (FINE, FINE)
NCH = len(FINE)
BEFORE = (
    "D1a5", "D1a1", "D1a0", "D1a2", "D1a3", "D1b1", "Wa0", "D1a4", "D1b0", "D1b3", "D1b2", "Sa0",
    "D2a1", "D1b4", "D2a3", "D2a5", "D2a0", "D1b5", "D2a4", "D2a2", "D3a5", "D3a3", "Sb0", "D3a1",
    "D3a4", "D3a0", "D3a2", "D2b1", "Wb0", "D2b0", "D2b3", "D2b5", "D2b2", "D2b4",
)
WHILE = {
    3: ("D3b1", "D3b5", "D3b0",),
    5: ("D3b2", "D3b4", "D3b3", "R1a0",),
    11: ("R1a1",),
    15: ("R2a2", "R2a1", "R2a0",),
    18: ("R2a5", "R1b0",),
    20: ("R2a3",),
    21: ("R2a4",),
    22: ("R3a2",),
}
AFTER = (
    "R1b1", "R3a4", "R3a0", "R2b2", "R2b0", "R2b5", "R3a5", "R2b3", "R3a3", "R2b1", "R3a1", "R2b4",
    "Ca3", "R3b0", "R3b1", "R3b2", "R3b3", "Ca5", "R3b4", "Ca0", "Ca1", "R3b5", "Ca2", "Cb1",
    "Ca4", "Cb0", "Cb2", "Cb4", "Cb3", "Cb5",
)


def moe_kernel(tok_a, tok_b, ids_a, ids_b, gate_a, gate_b, wg_in, wu_in, wd_in,
               out, relay_in, relay_out,
               idbuf, gath, gath_x, pairs, last, lift, x_last, out_last, comb_x, send2, rows, turn, fin, wg, wu, wd, hid, sel, comb,
               id_s, id_r, w_s, w_r, w_l, x_s, x_r,
               d1s, d1r, d2s, d2r, d3s, d3r, r1s, r1r, r2s, r2r, r3s, r3r):
    f32, bf16 = jnp.float32, jnp.bfloat16
    ep = lax.axis_index("ep")
    tp = lax.axis_index("tp")
    me = (ep // 16, lax.rem(ep // 4, 4), lax.rem(ep, 4))
    toks = (tok_a, tok_b)
    ids_n, gates_n = (ids_a, ids_b), (gate_a, gate_b)

    def shifted(axis, step):
        return lax.rem(me[axis] + step, 4)

    def peer(axis, step):
        return {"ep": ep + (shifted(axis, step) - me[axis]) * STRIDE[axis]}

    def remote(src, dst, s_sem, r_sem, dev):
        return pltpu.make_async_remote_copy(src, dst, s_sem, r_sem, device_id=dev, device_id_type=MESH_ID)

    def cols(chunk):
        return pl.ds(chunk[1], chunk[2])

    def fixed_canon(buf, bt, axis, at, chunk):
        if axis == 0:
            return buf.at[bt, at, :, :, :, cols(chunk)]
        if axis == 1:
            return buf.at[bt, :, at, :, :, cols(chunk)]
        return buf.at[bt, :, :, at, :, cols(chunk)]

    def relay_slot(buf, bt, o, chunk, at):
        if o == 2:
            return buf.at[bt, :, at, :, :, cols(chunk)]
        return buf.at[bt, :, :, at, :, cols(chunk)]

    def copy_d1(bt, k, i):
        o = IN[bt][k][0]
        return remote(toks[bt].at[:, cols(IN[bt][k])], gath.at[bt, me[o], :, cols(IN[bt][k])],
                      d1s.at[bt], d1r.at[bt, k], peer(o, i))

    def local_d1(bt, k):
        o = IN[bt][k][0]
        return pltpu.make_async_copy(toks[bt].at[:, cols(IN[bt][k])], gath.at[bt, me[o], :, cols(IN[bt][k])], d1r.at[bt, k])

    def copy_x(bt, o, i):
        return remote(toks[bt].at[:, pl.ds(MAIN, LANE)], gath_x.at[bt, o, me[o]],
                      x_s.at[bt], x_r.at[bt, o], peer(o, i))

    def local_x(bt, o):
        return pltpu.make_async_copy(toks[bt].at[:, pl.ds(MAIN, LANE)], gath_x.at[bt, o, me[o]], x_r.at[bt, o])

    def copy_d2(bt, k, i):
        o = IN[bt][k][0]
        b = (o + 1) % 3
        return remote(send2.at[shifted(b, i), :, :, :, cols(IN[bt][k])], relay_slot(relay_in, bt, o, IN[bt][k], me[b]),
                      d2s.at[bt], d2r.at[bt, k], peer(b, i))

    def local_d2(bt, k):
        o = IN[bt][k][0]
        b = (o + 1) % 3
        return pltpu.make_async_copy(send2.at[me[b], :, :, :, cols(IN[bt][k])], relay_slot(relay_in, bt, o, IN[bt][k], me[b]), d2r.at[bt, k])

    def copy_3(src, dst, s, r, chunk, bt, k, i):
        c = (chunk[0] + 2) % 3
        return remote(src.at[bt, shifted(c, i), :, :, :, cols(chunk)], fixed_canon(dst, bt, c, me[c], chunk),
                      s.at[bt], r.at[bt, k], peer(c, i))

    def local_3(src, dst, sem, chunk, bt, k):
        c = (chunk[0] + 2) % 3
        return pltpu.make_async_copy(src.at[bt, me[c], :, :, :, cols(chunk)], fixed_canon(dst, bt, c, me[c], chunk), sem.at[bt, k])

    far = 2 * (1 - me[0] // 2)

    def copy_r1(bt, k, i, h):
        o = OUT[bt][k][0]
        cs = cols(OUT[bt][k])
        planes = pl.ds(lax.rem(far + 2 * h, 4), 2)
        if o == 0:
            src, dst = rows.at[bt, shifted(0, i), :, :, :, cs], turn.at[bt, :, :, me[0], :, cs]
        elif o == 1:
            src, dst = rows.at[bt, planes, shifted(1, i), :, :, cs], turn.at[bt, planes, :, me[1], :, cs]
        else:
            src, dst = rows.at[bt, planes, :, shifted(2, i), :, cs], turn.at[bt, planes, :, me[2], :, cs]
        return remote(src, dst, r1s.at[bt], r1r.at[bt, k], peer(o, i))

    def turn_part(bt, k, at):
        if OUT[bt][k][0] == 1:
            return turn.at[bt, :, at, :, :, cols(OUT[bt][k])]
        return turn.at[bt, at, :, :, :, cols(OUT[bt][k])]

    def copy_r2(bt, k, i):
        o = OUT[bt][k][0]
        b = (o + 1) % 3
        return remote(turn_part(bt, k, shifted(b, i)), relay_slot(relay_out, bt, o, OUT[bt][k], me[b]),
                      r2s.at[bt], r2r.at[bt, k], peer(b, i))

    def local_r2(bt, k):
        o = OUT[bt][k][0]
        b = (o + 1) % 3
        return pltpu.make_async_copy(turn_part(bt, k, me[b]), relay_slot(relay_out, bt, o, OUT[bt][k], me[b]), r2r.at[bt, k])

    def copy_d3(bt, k, i):
        return copy_3(relay_in, rows, d3s, d3r, IN[bt][k], bt, k, i)

    def copy_r3(bt, k, i):
        return copy_3(relay_out, fin, r3s, r3r, OUT[bt][k], bt, k, i)

    def local_d3(bt, k):
        return local_3(relay_in, rows, d3r, IN[bt][k], bt, k)

    def local_r3(bt, k):
        return local_3(relay_out, fin, r3r, OUT[bt][k], bt, k)

    def start3(copy, bt, k):
        for i in (2, 1, 3):
            copy(bt, k, i).start()

    def drain(ref, sem):
        pltpu.make_async_copy(ref, ref, sem).wait()

    def arrived(buf, sem, bt, k, chunk):
        drain(buf.at[bt, :, :, :, :, cols(chunk)], sem.at[bt, k])

    def iota(shape, dim):
        return lax.broadcasted_iota(jnp.int32, shape, dim)

    def build_moves():
        row, col = iota((256, 256), 0), iota((256, 256), 1)
        pairs[...] = jnp.where(((row >> 4) == (col & 15)) & ((row & 15) == (col >> 4)), 1.0, 0.0).astype(bf16)
        last[...] = jnp.where(iota((128, 1024), 1) == iota((128, 1024), 0) * SLOT + CAP, 1.0, 0.0).astype(bf16)
        lift[...] = jnp.where(iota((256, SLOT), 0) == iota((256, SLOT), 1) * SLOT + CAP, 1.0, 0.0).astype(bf16)

    def fold(block, first, count):
        swapped = jnp.dot(pairs[...], block, preferred_element_type=f32).astype(bf16)
        parts = [swapped[j * SLOT:(j + 1) * SLOT] for j in range(first, first + count)]
        return jnp.concatenate(parts, axis=1)

    def build_comb(bt):
        ids, gates = ids_n[bt][...], gates_n[bt][...]
        expert = iota((64, TOK), 0)
        hit = jnp.zeros((64, TOK), f32)
        gate = jnp.zeros((64, TOK), f32)
        for j in range(6):
            same = ids[j:j + 1, :] == expert
            hit = jnp.where(same, 1.0, hit)
            gate = jnp.where(same, gates[j:j + 1, :], gate)
        before = jnp.where(iota((TOK, TOK), 0) < iota((TOK, TOK), 1), 1.0, 0.0).astype(bf16)
        count = jnp.dot(hit.astype(bf16), before, preferred_element_type=f32)
        place = jnp.transpose(jnp.where((hit > 0.5) & (count < CAP - 0.5), count, -1.0))
        gate = jnp.transpose(gate)
        spread = jnp.where((iota((64, 64 * SLOT), 1) >> 4) == iota((64, 64 * SLOT), 0), 1.0, 0.0).astype(bf16)
        wide = jnp.dot(place.astype(bf16), spread, preferred_element_type=f32)
        at_slot = wide == (iota((TOK, 64 * SLOT), 1) & 15).astype(f32)
        spread_x = jnp.where((iota((64, MAIN), 1) & 127) == iota((64, MAIN), 0), 1.0, 0.0).astype(bf16)
        wide_x = jnp.dot(place.astype(bf16), spread_x, preferred_element_type=f32)
        at_slot_x = wide_x == (iota((TOK, MAIN), 1) >> 7).astype(f32)
        rest = gate
        for n in range(3):
            part = rest.astype(bf16)
            rest = rest - part.astype(f32)
            part_wide = jnp.dot(part, spread, preferred_element_type=f32)
            comb[bt, n * TOK:(n + 1) * TOK, :] = jnp.where(at_slot, part_wide, 0.0).astype(bf16)
            part_wide = jnp.dot(part, spread_x, preferred_element_type=f32)
            comb_x[bt, n * TOK:(n + 1) * TOK, :] = jnp.where(at_slot_x, part_wide, 0.0).astype(bf16)

    def build_sel(bt):
        before = jnp.where(iota((TOK, TOK), 0) < iota((TOK, TOK), 1), 1.0, 0.0).astype(bf16)
        for o in range(3):
            b, c = (o + 1) % 3, (o + 2) % 3
            row = iota((16, TOK), 0)
            expert = me[o] * STRIDE[o] + (row >> 2) * STRIDE[b] + (row & 3) * STRIDE[c]
            for a in range(4):
                ids = idbuf[o, a, bt * 8:bt * 8 + 8, :]
                hit = jnp.zeros((16, TOK), f32)
                for j in range(6):
                    hit = jnp.where(ids[j:j + 1, :] == expert, 1.0, hit)
                count = jnp.dot(hit.astype(bf16), before, preferred_element_type=f32)
                place = jnp.where((hit > 0.5) & (count < CAP - 0.5), count, -1.0)
                slot = iota((SLOT, TOK), 0).astype(f32)
                for r in range(16):
                    sel[bt, o, a, r * SLOT:(r + 1) * SLOT, :] = jnp.where(place[r:r + 1, :] == slot, 1.0, 0.0).astype(bf16)

    barrier = pltpu.get_barrier_semaphore()
    for axis in range(3):
        for i in (1, 2, 3):
            pl.semaphore_signal(barrier, inc=1, device_id=peer(axis, i), device_id_type=MESH_ID)
    other = {"tp": 1 - tp}
    pl.semaphore_signal(barrier, inc=1, device_id=other, device_id_type=MESH_ID)
    for bt in (0, 1):
        for k in range(len(IN[bt])):
            local_d1(bt, k).start()
        for o in range(3):
            local_x(bt, o).start()
    weights = ((wg_in, wg), (wu_in, wu), (wd_in, wd))

    def weight_local(n):
        src, dst = weights[n]
        return pltpu.make_async_copy(src.at[0], dst.at[tp], w_l.at[n])

    def weight_remote(n):
        src, dst = weights[n]
        return remote(src.at[0], dst.at[tp], w_s.at[n], w_r.at[n], other)

    def id_copy(axis, i):
        return remote(idbuf.at[axis, me[axis]], idbuf.at[axis, me[axis]], id_s.at[0], id_r.at[0], peer(axis, i))

    for axis in range(3):
        idbuf[axis, me[axis]] = jnp.full((16, TOK), -1, jnp.int32)
        for bt in (0, 1):
            idbuf[axis, me[axis], bt * 8:bt * 8 + 6, :] = ids_n[bt][...]

    pl.semaphore_wait(barrier, 10)
    for axis in range(3):
        for i in (2, 1, 3):
            id_copy(axis, i).start()

    seen_x, sent_x, reused, left = set(), set(), [], [0, 0]

    def step_d2(bt, k):
        o, c0, w = IN[bt][k]
        drain(gath.at[bt, :, :, cols(IN[bt][k])], d1r.at[bt, k])
        if bt == 1 and not reused:
            reused.append(True)
            drain(send2.at[pl.ds(0, 3)], d2s.at[0])
        if (bt, o) not in seen_x:
            seen_x.add((bt, o))
            drain(gath_x.at[bt, o], x_r.at[bt, o])
        for a in range(4):
            tail = jnp.dot(sel[bt, o, a], gath_x[bt, o, a], preferred_element_type=f32).astype(bf16)
            got = jnp.dot(sel[bt, o, a], gath[bt, a, :, c0:c0 + w], preferred_element_type=f32)
            got = got + jnp.dot(lift[...], fold(tail, c0 // LANE, w // LANE), preferred_element_type=f32)
            send2[:, :, a, :, c0:c0 + w] = got.astype(bf16).reshape(4, 4, SLOT, w)
        start3(copy_d2, bt, k)
        local_d2(bt, k).start()

    def step_d3(bt, k):
        arrived(relay_in, d2r, bt, k, IN[bt][k])
        start3(copy_d3, bt, k)
        local_d3(bt, k).start()

    def wait_rows(bt):
        for k in range(len(IN[bt])):
            arrived(rows, d3r, bt, k, IN[bt][k])

    def expert_step(step):
        bt, part = step // 12, lax.rem(step, 3)
        m = lax.rem(far + lax.rem(step, 12) // 3, 4)

        @pl.when(part < 2)
        def _():
            x = rows[bt, m].reshape(256, MAIN)

            @pl.when(part == 0)
            def _():
                ends = jnp.dot(last[:SLOT, :256], x, preferred_element_type=f32).astype(bf16)
                tiles = [ends[:, j * LANE:(j + 1) * LANE] for j in range(CAP)] + [jnp.zeros((SLOT, LANE), bf16)]
                x_last[...] = jnp.dot(pairs[...], jnp.concatenate(tiles, axis=0), preferred_element_type=f32).astype(bf16)

            x = jnp.concatenate([x, x_last[...]], axis=1)
            g = lax.dot_general(x, wg[part], (((1,), (1,)), ((), ())), preferred_element_type=f32)
            u = lax.dot_general(x, wu[part], (((1,), (1,)), ((), ())), preferred_element_type=f32)
            hid[part] = (jax.nn.silu(g) * u).astype(bf16)

        @pl.when(part == 2)
        def _():
            total = jnp.dot(hid[0], wd[0], preferred_element_type=f32)
            total = total + jnp.dot(hid[1], wd[1], preferred_element_type=f32)
            folded = fold(total[:, MAIN:].astype(bf16), 0, CAP)
            lifted = jnp.dot(lift[...], folded, preferred_element_type=f32)
            kept = jnp.where((iota((256, MAIN), 0) & 15) == CAP, lifted, total[:, :MAIN])
            rows[bt, m] = kept.astype(bf16).reshape(4, 4, SLOT, MAIN)

    def step_d1(bt, k):
        o = IN[bt][k][0]
        if (bt, o) not in sent_x:
            sent_x.add((bt, o))
            start3(copy_x, bt, o)
        start3(copy_d1, bt, k)

    def step_r1(bt, h):
        for k in range(len(OUT[bt])):
            if OUT[bt][k][0] == 0:
                near = me[0] + 1 - 2 * lax.rem(me[0], 2)
                for z in (far, far + 1) if h == 0 else (near,):
                    copy_r1(bt, k, lax.rem(z - me[0] + 4, 4), 0).start()
            else:
                for i in (2, 1, 3):
                    copy_r1(bt, k, i, h).start()
        planes = pl.ds(lax.rem(far + 2 * h, 4), 2)
        for o, c0, w in OUT[bt]:
            cs = slice(c0, c0 + w)
            if o == 0 and h == 1:
                turn[bt, :, :, me[0], :, cs] = rows[bt, me[0], :, :, :, cs]
            elif o == 1:
                turn[bt, planes, :, me[1], :, cs] = rows[bt, planes, me[1], :, :, cs]
            elif o == 2:
                turn[bt, planes, :, me[2], :, cs] = rows[bt, planes, :, me[2], :, cs]

    def step_r2(bt, k):
        drain(turn.at[bt, pl.ds(0, 3), :, :, :, cols(OUT[bt][k])], r1r.at[bt, k])
        start3(copy_r2, bt, k)
        local_r2(bt, k).start()

    def step_r3(bt, k):
        arrived(relay_out, r2r, bt, k, OUT[bt][k])
        start3(copy_r3, bt, k)
        local_r3(bt, k).start()

    def step_out(bt, k):
        o, c0, w = OUT[bt][k]
        arrived(fin, r3r, bt, k, OUT[bt][k])
        vals = fin[bt, :, :, :, :, c0:c0 + w].reshape(64 * SLOT, w)
        got = jnp.dot(comb[bt], vals, preferred_element_type=f32)
        out[bt, :, c0:c0 + w] = (got[:TOK] + got[TOK:2 * TOK] + got[2 * TOK:]).astype(bf16)
        ends = jnp.dot(last[...], vals, preferred_element_type=f32).astype(bf16)
        tiles = jnp.concatenate([ends[:, j * LANE:(j + 1) * LANE] for j in range(w // LANE)], axis=0)
        got = jnp.dot(comb_x[bt, :, c0:c0 + w], tiles, preferred_element_type=f32)
        total = got[:TOK] + got[TOK:2 * TOK] + got[2 * TOK:]
        if left[bt]:
            total = out_last[bt] + total
        left[bt] += 1
        if left[bt] < len(OUT[bt]):
            out_last[bt] = total
        else:
            out[bt, :, MAIN:] = total.astype(bf16)

    todo = {"D1": step_d1, "D2": step_d2, "D3": step_d3, "R1": step_r1, "R2": step_r2, "R3": step_r3, "C": step_out,
            "S": lambda bt, k: build_sel(bt), "W": lambda bt, k: build_comb(bt)}

    def run(steps):
        for step in steps:
            name, bt, k = step[:-2], "ab".index(step[-2]), int(step[-1])
            if (name, bt) == ("S", 0):
                for n in range(3):
                    weight_local(n).start()
                    weight_remote(n).start()
                build_moves()
                drain(idbuf.at[:, pl.ds(0, 3)], id_r.at[0])
            todo[name](bt, k)

    run(BEFORE)
    for n in range(3):
        weight_local(n).wait()
        weight_remote(n).wait_recv()
    wait_rows(0)

    def loop(step, carry):
        @pl.when(step == 12)
        def _():
            wait_rows(1)

        expert_step(step)
        for at, steps in WHILE.items():
            @pl.when(step == at)
            def _():
                run(steps)
        return carry

    lax.fori_loop(0, 24, loop, 0)
    run(AFTER)

    drain(idbuf.at[:, pl.ds(0, 3)], id_s.at[0])
    for n in range(3):
        weight_remote(n).wait_send()
    drain(send2.at[pl.ds(0, 3)], d2s.at[1])
    for bt in (0, 1):
        drain(gath.at[bt, pl.ds(0, 3)], d1s.at[bt])
        drain(gath_x.at[bt, :, pl.ds(0, 3)], x_s.at[bt])
        drain(rows.at[bt, pl.ds(0, 3)], d3s.at[bt])
        drain(rows.at[bt, pl.ds(0, 3)], r1s.at[bt])
        drain(turn.at[bt, pl.ds(0, 3)], r2s.at[bt])
        drain(fin.at[bt, pl.ds(0, 3)], r3s.at[bt])


def solution(mesh):
    row_spec = P(("dp", "ep", "tp"), None)
    gate_spec = P("ep", None, "tp")
    down_spec = P("ep", "tp", None)
    bf16 = jnp.bfloat16
    dma = pltpu.SemaphoreType.DMA

    def body(tok_a, ids_a, gate_a, tok_b, ids_b, gate_b, wg, wu, wd):
        vmem = pl.BlockSpec(memory_space=pltpu.VMEM)
        hbm = pl.BlockSpec(memory_space=pl.ANY)
        half = wd.shape[1]
        box = (2, 4, 4, 4, SLOT, MAIN)
        out = jax.ShapeDtypeStruct((TOK, DIM), bf16)
        relay = jax.ShapeDtypeStruct(box, bf16)
        res = pl.pallas_call(
            moe_kernel,
            out_shape=(jax.ShapeDtypeStruct((2, TOK, DIM), bf16), relay, relay),
            in_specs=[hbm, hbm, vmem, vmem, vmem, vmem, hbm, hbm, hbm],
            out_specs=(vmem, hbm, hbm),
            scratch_shapes=[
                pltpu.VMEM((3, 4, 16, TOK), jnp.int32),
                pltpu.VMEM((2, 4, TOK, MAIN), bf16),
                pltpu.VMEM((2, 3, 4, TOK, LANE), bf16),
                pltpu.VMEM((256, 256), bf16),
                pltpu.VMEM((128, 1024), bf16),
                pltpu.VMEM((256, SLOT), bf16),
                pltpu.VMEM((256, LANE), bf16),
                pltpu.VMEM((2, TOK, LANE), jnp.float32),
                pltpu.VMEM((2, 3 * TOK, MAIN), bf16),
                pltpu.VMEM((4, 4, 4, SLOT, MAIN), bf16),
                pltpu.VMEM(box, bf16),
                pltpu.VMEM(box, bf16),
                pltpu.VMEM(box, bf16),
                pltpu.VMEM((2, half, DIM), bf16),
                pltpu.VMEM((2, half, DIM), bf16),
                pltpu.VMEM((2, half, DIM), bf16),
                pltpu.VMEM((2, 256, half), bf16),
                pltpu.VMEM((2, 3, 4, 256, TOK), bf16),
                pltpu.VMEM((2, 3 * TOK, 64 * SLOT), bf16),
                dma((1,)), dma((1,)), dma((3,)), dma((3,)), dma((3,)), dma((2,)), dma((2, 3)),
                *([dma((2,)), dma((2, NCH))] * 6),
            ],
            compiler_params=pltpu.CompilerParams(collective_id=0, has_side_effects=True, vmem_limit_bytes=67043328),
            name="moe",
        )(tok_a, tok_b, ids_a.T, ids_b.T, gate_a.T, gate_b.T, wg.transpose(0, 2, 1), wu.transpose(0, 2, 1), wd)
        return res[0][0], res[0][1]

    specs = (row_spec,) * 6 + (gate_spec, gate_spec, down_spec)
    return jax.shard_map(body, mesh=mesh, in_specs=specs, out_specs=(row_spec, row_spec), check_vma=False)
```

```python
import jax
import jax.numpy as jnp
from jax import lax
from jax.experimental import pallas as pl
from jax.experimental.pallas import tpu as pltpu
from jax.sharding import PartitionSpec as P

MESH_ID = pl.DeviceIdType.MESH
SLOT = 16
CAP = 15
TOK = 128
DIM = 2048
MAIN = 1920
LANE = 128
STRIDE = (16, 4, 1)
FINE = ((0, 0, 384), (1, 384, 384), (2, 768, 384), (0, 1152, 256), (1, 1408, 256), (2, 1664, 256))
COARSE = ((0, 0, 640), (1, 640, 640), (2, 1280, 640))
IN, OUT = (FINE, FINE), (FINE, FINE)
NCH = len(FINE)
BEFORE = (
    "D1a5", "D1a1", "D1a0", "D1a2", "D1a3", "D1b1", "Wa0", "D1a4", "D1b0", "D1b3", "D1b2", "Sa0",
    "D2a1", "D1b4", "D2a3", "D2a5", "D2a0", "D1b5", "D2a4", "D2a2", "D3a5", "D3a3", "Sb0", "D3a1",
    "D3a4", "D3a0", "D3a2", "D2b1", "Wb0", "D2b0", "D2b3", "D2b5", "D2b2", "D2b4",
)
WHILE = {
    3: ("D3b1", "D3b5", "D3b0",),
    5: ("D3b2", "D3b4", "D3b3", "R1a0",),
    11: ("R1a1",),
    15: ("R2a2", "R2a1", "R2a0",),
    18: ("R2a5", "R1b0",),
    20: ("R2a3",),
    21: ("R2a4",),
    22: ("R3a2",),
}
AFTER = (
    "R1b1", "R3a4", "R3a0", "R2b2", "R2b0", "R2b5", "R3a5", "R2b3", "R3a3", "R2b1", "R3a1", "R2b4",
    "Ca3", "R3b0", "R3b1", "R3b2", "R3b3", "Ca5", "R3b4", "Ca0", "Ca1", "R3b5", "Ca2", "Cb1",
    "Ca4", "Cb0", "Cb2", "Cb4", "Cb3", "Cb5",
)


def moe_kernel(tok_a, tok_b, ids_a, ids_b, gate_a, gate_b, wg_in, wu_in, wd_in,
               out, relay_in, relay_out,
               idbuf, gath, gath_x, pairs, last, lift, x_last, out_last, comb_x, send2, rows, turn, fin, wg, wu, wd, hid, sel, comb,
               id_s, id_r, w_s, w_r, w_l, x_s, x_r,
               d1s, d1r, d2s, d2r, d3s, d3r, r1s, r1r, r2s, r2r, r3s, r3r):
    f32, bf16 = jnp.float32, jnp.bfloat16
    ep = lax.axis_index("ep")
    tp = lax.axis_index("tp")
    me = (ep // 16, lax.rem(ep // 4, 4), lax.rem(ep, 4))
    toks = (tok_a, tok_b)
    ids_n, gates_n = (ids_a, ids_b), (gate_a, gate_b)

    def shifted(axis, step):
        return lax.rem(me[axis] + step, 4)

    def peer(axis, step):
        return {"ep": ep + (shifted(axis, step) - me[axis]) * STRIDE[axis]}

    def remote(src, dst, s_sem, r_sem, dev):
        return pltpu.make_async_remote_copy(src, dst, s_sem, r_sem, device_id=dev, device_id_type=MESH_ID)

    def cols(chunk):
        return pl.ds(chunk[1], chunk[2])

    def fixed_canon(buf, bt, axis, at, chunk):
        if axis == 0:
            return buf.at[bt, at, :, :, :, cols(chunk)]
        if axis == 1:
            return buf.at[bt, :, at, :, :, cols(chunk)]
        return buf.at[bt, :, :, at, :, cols(chunk)]

    def relay_slot(buf, bt, o, chunk, at):
        if o == 2:
            return buf.at[bt, :, at, :, :, cols(chunk)]
        return buf.at[bt, :, :, at, :, cols(chunk)]

    def copy_d1(bt, k, i):
        o = IN[bt][k][0]
        return remote(toks[bt].at[:, cols(IN[bt][k])], gath.at[bt, me[o], :, cols(IN[bt][k])],
                      d1s.at[bt], d1r.at[bt, k], peer(o, i))

    def local_d1(bt, k):
        o = IN[bt][k][0]
        return pltpu.make_async_copy(toks[bt].at[:, cols(IN[bt][k])], gath.at[bt, me[o], :, cols(IN[bt][k])], d1r.at[bt, k])

    def copy_x(bt, o, i):
        return remote(toks[bt].at[:, pl.ds(MAIN, LANE)], gath_x.at[bt, o, me[o]],
                      x_s.at[bt], x_r.at[bt, o], peer(o, i))

    def local_x(bt, o):
        return pltpu.make_async_copy(toks[bt].at[:, pl.ds(MAIN, LANE)], gath_x.at[bt, o, me[o]], x_r.at[bt, o])

    def copy_d2(bt, k, i):
        o = IN[bt][k][0]
        b = (o + 1) % 3
        return remote(send2.at[shifted(b, i), :, :, :, cols(IN[bt][k])], relay_slot(relay_in, bt, o, IN[bt][k], me[b]),
                      d2s.at[bt], d2r.at[bt, k], peer(b, i))

    def local_d2(bt, k):
        o = IN[bt][k][0]
        b = (o + 1) % 3
        return pltpu.make_async_copy(send2.at[me[b], :, :, :, cols(IN[bt][k])], relay_slot(relay_in, bt, o, IN[bt][k], me[b]), d2r.at[bt, k])

    def copy_3(src, dst, s, r, chunk, bt, k, i):
        c = (chunk[0] + 2) % 3
        return remote(src.at[bt, shifted(c, i), :, :, :, cols(chunk)], fixed_canon(dst, bt, c, me[c], chunk),
                      s.at[bt], r.at[bt, k], peer(c, i))

    def local_3(src, dst, sem, chunk, bt, k):
        c = (chunk[0] + 2) % 3
        return pltpu.make_async_copy(src.at[bt, me[c], :, :, :, cols(chunk)], fixed_canon(dst, bt, c, me[c], chunk), sem.at[bt, k])

    far = 2 * (1 - me[0] // 2)

    def copy_r1(bt, k, i, h):
        o = OUT[bt][k][0]
        cs = cols(OUT[bt][k])
        planes = pl.ds(lax.rem(far + 2 * h, 4), 2)
        if o == 0:
            src, dst = rows.at[bt, shifted(0, i), :, :, :, cs], turn.at[bt, :, :, me[0], :, cs]
        elif o == 1:
            src, dst = rows.at[bt, planes, shifted(1, i), :, :, cs], turn.at[bt, planes, :, me[1], :, cs]
        else:
            src, dst = rows.at[bt, planes, :, shifted(2, i), :, cs], turn.at[bt, planes, :, me[2], :, cs]
        return remote(src, dst, r1s.at[bt], r1r.at[bt, k], peer(o, i))

    def turn_part(bt, k, at):
        if OUT[bt][k][0] == 1:
            return turn.at[bt, :, at, :, :, cols(OUT[bt][k])]
        return turn.at[bt, at, :, :, :, cols(OUT[bt][k])]

    def copy_r2(bt, k, i):
        o = OUT[bt][k][0]
        b = (o + 1) % 3
        return remote(turn_part(bt, k, shifted(b, i)), relay_slot(relay_out, bt, o, OUT[bt][k], me[b]),
                      r2s.at[bt], r2r.at[bt, k], peer(b, i))

    def local_r2(bt, k):
        o = OUT[bt][k][0]
        b = (o + 1) % 3
        return pltpu.make_async_copy(turn_part(bt, k, me[b]), relay_slot(relay_out, bt, o, OUT[bt][k], me[b]), r2r.at[bt, k])

    def copy_d3(bt, k, i):
        return copy_3(relay_in, rows, d3s, d3r, IN[bt][k], bt, k, i)

    def copy_r3(bt, k, i):
        return copy_3(relay_out, fin, r3s, r3r, OUT[bt][k], bt, k, i)

    def local_d3(bt, k):
        return local_3(relay_in, rows, d3r, IN[bt][k], bt, k)

    def local_r3(bt, k):
        return local_3(relay_out, fin, r3r, OUT[bt][k], bt, k)

    def start3(copy, bt, k):
        for i in (1, 3, 2):
            copy(bt, k, i).start()

    def drain(ref, sem):
        pltpu.make_async_copy(ref, ref, sem).wait()

    def arrived(buf, sem, bt, k, chunk):
        drain(buf.at[bt, :, :, :, :, cols(chunk)], sem.at[bt, k])

    def iota(shape, dim):
        return lax.broadcasted_iota(jnp.int32, shape, dim)

    def build_moves():
        row, col = iota((256, 256), 0), iota((256, 256), 1)
        pairs[...] = jnp.where(((row >> 4) == (col & 15)) & ((row & 15) == (col >> 4)), 1.0, 0.0).astype(bf16)
        last[...] = jnp.where(iota((128, 1024), 1) == iota((128, 1024), 0) * SLOT + CAP, 1.0, 0.0).astype(bf16)
        lift[...] = jnp.where(iota((256, SLOT), 0) == iota((256, SLOT), 1) * SLOT + CAP, 1.0, 0.0).astype(bf16)

    def fold(block, first, count):
        swapped = jnp.dot(pairs[...], block, preferred_element_type=f32).astype(bf16)
        parts = [swapped[j * SLOT:(j + 1) * SLOT] for j in range(first, first + count)]
        return jnp.concatenate(parts, axis=1)

    def build_comb(bt):
        ids, gates = ids_n[bt][...], gates_n[bt][...]
        expert = iota((64, TOK), 0)
        hit = jnp.zeros((64, TOK), f32)
        gate = jnp.zeros((64, TOK), f32)
        for j in range(6):
            same = ids[j:j + 1, :] == expert
            hit = jnp.where(same, 1.0, hit)
            gate = jnp.where(same, gates[j:j + 1, :], gate)
        before = jnp.where(iota((TOK, TOK), 0) < iota((TOK, TOK), 1), 1.0, 0.0).astype(bf16)
        count = jnp.dot(hit.astype(bf16), before, preferred_element_type=f32)
        place = jnp.transpose(jnp.where((hit > 0.5) & (count < CAP - 0.5), count, -1.0))
        gate = jnp.transpose(gate)
        spread = jnp.where((iota((64, 64 * SLOT), 1) >> 4) == iota((64, 64 * SLOT), 0), 1.0, 0.0).astype(bf16)
        wide = jnp.dot(place.astype(bf16), spread, preferred_element_type=f32)
        at_slot = wide == (iota((TOK, 64 * SLOT), 1) & 15).astype(f32)
        spread_x = jnp.where((iota((64, MAIN), 1) & 127) == iota((64, MAIN), 0), 1.0, 0.0).astype(bf16)
        wide_x = jnp.dot(place.astype(bf16), spread_x, preferred_element_type=f32)
        at_slot_x = wide_x == (iota((TOK, MAIN), 1) >> 7).astype(f32)
        rest = gate
        for n in range(3):
            part = rest.astype(bf16)
            rest = rest - part.astype(f32)
            part_wide = jnp.dot(part, spread, preferred_element_type=f32)
            comb[bt, n * TOK:(n + 1) * TOK, :] = jnp.where(at_slot, part_wide, 0.0).astype(bf16)
            part_wide = jnp.dot(part, spread_x, preferred_element_type=f32)
            comb_x[bt, n * TOK:(n + 1) * TOK, :] = jnp.where(at_slot_x, part_wide, 0.0).astype(bf16)

    def build_sel(bt):
        before = jnp.where(iota((TOK, TOK), 0) < iota((TOK, TOK), 1), 1.0, 0.0).astype(bf16)
        for o in range(3):
            b, c = (o + 1) % 3, (o + 2) % 3
            row = iota((16, TOK), 0)
            expert = me[o] * STRIDE[o] + (row >> 2) * STRIDE[b] + (row & 3) * STRIDE[c]
            for a in range(4):
                ids = idbuf[o, a, bt * 8:bt * 8 + 8, :]
                hit = jnp.zeros((16, TOK), f32)
                for j in range(6):
                    hit = jnp.where(ids[j:j + 1, :] == expert, 1.0, hit)
                count = jnp.dot(hit.astype(bf16), before, preferred_element_type=f32)
                place = jnp.where((hit > 0.5) & (count < CAP - 0.5), count, -1.0)
                slot = iota((SLOT, TOK), 0).astype(f32)
                for r in range(16):
                    sel[bt, o, a, r * SLOT:(r + 1) * SLOT, :] = jnp.where(place[r:r + 1, :] == slot, 1.0, 0.0).astype(bf16)

    barrier = pltpu.get_barrier_semaphore()
    for axis in range(3):
        for i in (1, 2, 3):
            pl.semaphore_signal(barrier, inc=1, device_id=peer(axis, i), device_id_type=MESH_ID)
    other = {"tp": 1 - tp}
    pl.semaphore_signal(barrier, inc=1, device_id=other, device_id_type=MESH_ID)
    for bt in (0, 1):
        for k in range(len(IN[bt])):
            local_d1(bt, k).start()
        for o in range(3):
            local_x(bt, o).start()
    weights = ((wg_in, wg), (wu_in, wu), (wd_in, wd))

    def weight_local(n):
        src, dst = weights[n]
        return pltpu.make_async_copy(src.at[0], dst.at[tp], w_l.at[n])

    def weight_remote(n):
        src, dst = weights[n]
        return remote(src.at[0], dst.at[tp], w_s.at[n], w_r.at[n], other)

    def id_copy(axis, i):
        return remote(idbuf.at[axis, me[axis]], idbuf.at[axis, me[axis]], id_s.at[0], id_r.at[0], peer(axis, i))

    for axis in range(3):
        idbuf[axis, me[axis]] = jnp.full((16, TOK), -1, jnp.int32)
        for bt in (0, 1):
            idbuf[axis, me[axis], bt * 8:bt * 8 + 6, :] = ids_n[bt][...]

    pl.semaphore_wait(barrier, 10)
    for axis in range(3):
        for i in (2, 1, 3):
            id_copy(axis, i).start()

    seen_x, sent_x, reused, left = set(), set(), [], [0, 0]

    def step_d2(bt, k):
        o, c0, w = IN[bt][k]
        drain(gath.at[bt, :, :, cols(IN[bt][k])], d1r.at[bt, k])
        if bt == 1 and not reused:
            reused.append(True)
            drain(send2.at[pl.ds(0, 3)], d2s.at[0])
        if (bt, o) not in seen_x:
            seen_x.add((bt, o))
            drain(gath_x.at[bt, o], x_r.at[bt, o])
        for a in range(4):
            tail = jnp.dot(sel[bt, o, a], gath_x[bt, o, a], preferred_element_type=f32).astype(bf16)
            got = jnp.dot(sel[bt, o, a], gath[bt, a, :, c0:c0 + w], preferred_element_type=f32)
            got = got + jnp.dot(lift[...], fold(tail, c0 // LANE, w // LANE), preferred_element_type=f32)
            send2[:, :, a, :, c0:c0 + w] = got.astype(bf16).reshape(4, 4, SLOT, w)
        start3(copy_d2, bt, k)
        local_d2(bt, k).start()

    def step_d3(bt, k):
        arrived(relay_in, d2r, bt, k, IN[bt][k])
        start3(copy_d3, bt, k)
        local_d3(bt, k).start()

    def wait_rows(bt):
        for k in range(len(IN[bt])):
            arrived(rows, d3r, bt, k, IN[bt][k])

    def expert_step(step):
        bt, part = step // 12, lax.rem(step, 3)
        m = lax.rem(far + lax.rem(step, 12) // 3, 4)

        @pl.when(part < 2)
        def _():
            x = rows[bt, m].reshape(256, MAIN)

            @pl.when(part == 0)
            def _():
                ends = jnp.dot(last[:SLOT, :256], x, preferred_element_type=f32).astype(bf16)
                tiles = [ends[:, j * LANE:(j + 1) * LANE] for j in range(CAP)] + [jnp.zeros((SLOT, LANE), bf16)]
                x_last[...] = jnp.dot(pairs[...], jnp.concatenate(tiles, axis=0), preferred_element_type=f32).astype(bf16)

            x = jnp.concatenate([x, x_last[...]], axis=1)
            g = lax.dot_general(x, wg[part], (((1,), (1,)), ((), ())), preferred_element_type=f32)
            u = lax.dot_general(x, wu[part], (((1,), (1,)), ((), ())), preferred_element_type=f32)
            hid[part] = (jax.nn.silu(g) * u).astype(bf16)

        @pl.when(part == 2)
        def _():
            total = jnp.dot(hid[0], wd[0], preferred_element_type=f32)
            total = total + jnp.dot(hid[1], wd[1], preferred_element_type=f32)
            folded = fold(total[:, MAIN:].astype(bf16), 0, CAP)
            lifted = jnp.dot(lift[...], folded, preferred_element_type=f32)
            kept = jnp.where((iota((256, MAIN), 0) & 15) == CAP, lifted, total[:, :MAIN])
            rows[bt, m] = kept.astype(bf16).reshape(4, 4, SLOT, MAIN)

    def step_d1(bt, k):
        o = IN[bt][k][0]
        if (bt, o) not in sent_x:
            sent_x.add((bt, o))
            start3(copy_x, bt, o)
        start3(copy_d1, bt, k)

    def step_r1(bt, h):
        for k in range(len(OUT[bt])):
            if OUT[bt][k][0] == 0:
                near = me[0] + 1 - 2 * lax.rem(me[0], 2)
                for z in (far, far + 1) if h == 0 else (near,):
                    copy_r1(bt, k, lax.rem(z - me[0] + 4, 4), 0).start()
            else:
                for i in (2, 1, 3):
                    copy_r1(bt, k, i, h).start()
        planes = pl.ds(lax.rem(far + 2 * h, 4), 2)
        for o, c0, w in OUT[bt]:
            cs = slice(c0, c0 + w)
            if o == 0 and h == 1:
                turn[bt, :, :, me[0], :, cs] = rows[bt, me[0], :, :, :, cs]
            elif o == 1:
                turn[bt, planes, :, me[1], :, cs] = rows[bt, planes, me[1], :, :, cs]
            elif o == 2:
                turn[bt, planes, :, me[2], :, cs] = rows[bt, planes, :, me[2], :, cs]

    def step_r2(bt, k):
        drain(turn.at[bt, pl.ds(0, 3), :, :, :, cols(OUT[bt][k])], r1r.at[bt, k])
        start3(copy_r2, bt, k)
        local_r2(bt, k).start()

    def step_r3(bt, k):
        arrived(relay_out, r2r, bt, k, OUT[bt][k])
        start3(copy_r3, bt, k)
        local_r3(bt, k).start()

    def step_out(bt, k):
        o, c0, w = OUT[bt][k]
        arrived(fin, r3r, bt, k, OUT[bt][k])
        vals = fin[bt, :, :, :, :, c0:c0 + w].reshape(64 * SLOT, w)
        got = jnp.dot(comb[bt], vals, preferred_element_type=f32)
        out[bt, :, c0:c0 + w] = (got[:TOK] + got[TOK:2 * TOK] + got[2 * TOK:]).astype(bf16)
        ends = jnp.dot(last[...], vals, preferred_element_type=f32).astype(bf16)
        tiles = jnp.concatenate([ends[:, j * LANE:(j + 1) * LANE] for j in range(w // LANE)], axis=0)
        got = jnp.dot(comb_x[bt, :, c0:c0 + w], tiles, preferred_element_type=f32)
        total = got[:TOK] + got[TOK:2 * TOK] + got[2 * TOK:]
        if left[bt]:
            total = out_last[bt] + total
        left[bt] += 1
        if left[bt] < len(OUT[bt]):
            out_last[bt] = total
        else:
            out[bt, :, MAIN:] = total.astype(bf16)

    todo = {"D1": step_d1, "D2": step_d2, "D3": step_d3, "R1": step_r1, "R2": step_r2, "R3": step_r3, "C": step_out,
            "S": lambda bt, k: build_sel(bt), "W": lambda bt, k: build_comb(bt)}

    swapped = []

    def run(steps):
        for step in steps:
            name, bt, k = step[:-2], "ab".index(step[-2]), int(step[-1])
            if (name, bt) == ("D3", 0) and not swapped:
                swapped.append(True)
                for n in range(3):
                    weight_local(n).start()
                    weight_remote(n).start()
            if (name, bt) == ("S", 0):
                build_moves()
                drain(idbuf.at[:, pl.ds(0, 3)], id_r.at[0])
            todo[name](bt, k)

    run(BEFORE)
    for n in range(3):
        weight_local(n).wait()
        weight_remote(n).wait_recv()
    wait_rows(0)

    def loop(step, carry):
        @pl.when(step == 12)
        def _():
            wait_rows(1)

        expert_step(step)
        for at, steps in WHILE.items():
            @pl.when(step == at)
            def _():
                run(steps)
        return carry

    lax.fori_loop(0, 24, loop, 0)
    run(AFTER)

    drain(idbuf.at[:, pl.ds(0, 3)], id_s.at[0])
    for n in range(3):
        weight_remote(n).wait_send()
    drain(send2.at[pl.ds(0, 3)], d2s.at[1])
    for bt in (0, 1):
        drain(gath.at[bt, pl.ds(0, 3)], d1s.at[bt])
        drain(gath_x.at[bt, :, pl.ds(0, 3)], x_s.at[bt])
        drain(rows.at[bt, pl.ds(0, 3)], d3s.at[bt])
        drain(rows.at[bt, pl.ds(0, 3)], r1s.at[bt])
        drain(turn.at[bt, pl.ds(0, 3)], r2s.at[bt])
        drain(fin.at[bt, pl.ds(0, 3)], r3s.at[bt])


def solution(mesh):
    row_spec = P(("dp", "ep", "tp"), None)
    gate_spec = P("ep", None, "tp")
    down_spec = P("ep", "tp", None)
    bf16 = jnp.bfloat16
    dma = pltpu.SemaphoreType.DMA

    def body(tok_a, ids_a, gate_a, tok_b, ids_b, gate_b, wg, wu, wd):
        vmem = pl.BlockSpec(memory_space=pltpu.VMEM)
        hbm = pl.BlockSpec(memory_space=pl.ANY)
        half = wd.shape[1]
        box = (2, 4, 4, 4, SLOT, MAIN)
        out = jax.ShapeDtypeStruct((TOK, DIM), bf16)
        relay = jax.ShapeDtypeStruct(box, bf16)
        res = pl.pallas_call(
            moe_kernel,
            out_shape=(jax.ShapeDtypeStruct((2, TOK, DIM), bf16), relay, relay),
            in_specs=[hbm, hbm, vmem, vmem, vmem, vmem, hbm, hbm, hbm],
            out_specs=(vmem, hbm, hbm),
            scratch_shapes=[
                pltpu.VMEM((3, 4, 16, TOK), jnp.int32),
                pltpu.VMEM((2, 4, TOK, MAIN), bf16),
                pltpu.VMEM((2, 3, 4, TOK, LANE), bf16),
                pltpu.VMEM((256, 256), bf16),
                pltpu.VMEM((128, 1024), bf16),
                pltpu.VMEM((256, SLOT), bf16),
                pltpu.VMEM((256, LANE), bf16),
                pltpu.VMEM((2, TOK, LANE), jnp.float32),
                pltpu.VMEM((2, 3 * TOK, MAIN), bf16),
                pltpu.VMEM((4, 4, 4, SLOT, MAIN), bf16),
                pltpu.VMEM(box, bf16),
                pltpu.VMEM(box, bf16),
                pltpu.VMEM(box, bf16),
                pltpu.VMEM((2, half, DIM), bf16),
                pltpu.VMEM((2, half, DIM), bf16),
                pltpu.VMEM((2, half, DIM), bf16),
                pltpu.VMEM((2, 256, half), bf16),
                pltpu.VMEM((2, 3, 4, 256, TOK), bf16),
                pltpu.VMEM((2, 3 * TOK, 64 * SLOT), bf16),
                dma((1,)), dma((1,)), dma((3,)), dma((3,)), dma((3,)), dma((2,)), dma((2, 3)),
                *([dma((2,)), dma((2, NCH))] * 6),
            ],
            compiler_params=pltpu.CompilerParams(collective_id=0, has_side_effects=True, vmem_limit_bytes=67043328),
            name="moe",
        )(tok_a, tok_b, ids_a.T, ids_b.T, gate_a.T, gate_b.T, wg.transpose(0, 2, 1), wu.transpose(0, 2, 1), wd)
        return res[0][0], res[0][1]

    specs = (row_spec,) * 6 + (gate_spec, gate_spec, down_spec)
    return jax.shard_map(body, mesh=mesh, in_specs=specs, out_specs=(row_spec, row_spec), check_vma=False)
```
